512 devices in a mesh: rows: 64 (over y, z), inner: 8 (over x, core).
Axes of the slice: x: 4, y: 8, z: 8, core: 2. Of those that a mesh axis runs over, the one named last changes fastest.
Arguments:
- r_tiles: bfloat16 [512, 64, 128, 128], P('rows', 'inner'), may hold values from -0.5 to 0.5
- r_cols: int32 [512, 64], P('rows', 'inner'), may hold values from 0 to 4095, as said below
- a_tiles: bfloat16 [4096, 7, 128, 128], P(('rows', 'inner')), may hold values from -6 to 6
- a_cols: int32 [4096, 7], replicated, may hold values from 0 to 4095, as said below
- c_cols: int32 [512, 8], P('rows'), may hold values from -1 to 4095, as said below
- c_counts: int32 [512], P('rows'), may hold values from 4 to 8, as said below
Outputs:
- c_tiles: bfloat16 [512, 8, 128, 128], P('rows', 'inner')
- row_offsets: int32 [512], P('rows')
The draws below stay inside these ranges and needn't reach their ends.
Inputs may be any that keep to these rules, and one draw needn't show every extreme that they name: `r_cols`: the slots g * 8 to (g + 1) * 8 - 1 of block row c name distinct fine block rows k with (k // 8) % 8 == g and k // 64 within one of c // 8. `a_cols`: row k names 7 distinct fine block columns, the first of them k. `c_cols`: the first c_counts[c] entries of row c are distinct block columns, the others are -1. `c_counts`: each aligned group of 8 block rows has one with 8 live slots.
All inputs are finite; a program needn't handle non-finite values.
Results may differ from the reference program's by a relative error of at most 0.001.
Values may be sent and summed in bfloat16 or wider, within the bound.
No kernel may reach another device: no remote copies, remote signals or barrier semaphores. Data moves between devices by JAX's collectives and lax.ppermute only.
A program may use at most 64 MiB of HBM per device.

```python
import jax
import jax.numpy as jnp
from jax import lax

TB = 128
RB_DEV = 8
SR_DEV = 8
KA_DEV = 8
SA = 7
CAP = 8
NCB = 512
SR = 64
NK = 4096
N_ROWS = 64
N_INNER = 8


def pattern(key):
    span = 3 * KA_DEV
    coarse_owner = jnp.arange(NCB, dtype=jnp.int32) // RB_DEV
    candidate = jnp.arange(span, dtype=jnp.int32)
    shift_rows = candidate // KA_DEV - 1
    neighbour = coarse_owner[:, None, None] + shift_rows[None, None, :]
    usable = (neighbour >= 0) & (neighbour < N_ROWS)
    group_ids = jnp.arange(N_INNER, dtype=jnp.int32)
    noise_r = jax.random.randint(jax.random.fold_in(key, 101), (NCB, N_INNER, span), 0, 65536)
    scores = noise_r * span + candidate[None, None, :]
    scores = jnp.where((candidate == 0)[None, None, :] & usable, -2, scores)
    scores = jnp.where((candidate == 2 * KA_DEV)[None, None, :] & usable, -1, scores)
    scores = jnp.where(usable, scores, 2 ** 30)
    chosen_q = jnp.argsort(scores, axis=-1)[:, :, :SR_DEV].astype(jnp.int32)
    chosen_shift = chosen_q // KA_DEV - 1
    chosen_local = chosen_q % KA_DEV
    fine_rows = ((coarse_owner[:, None, None] + chosen_shift) * N_INNER + group_ids[None, :, None]) * KA_DEV + chosen_local
    r_columns = fine_rows.reshape(NCB, SR).astype(jnp.int32)
    first_stride = jax.random.randint(jax.random.fold_in(key, 606), (), 9, 17).astype(jnp.int32)
    second_raw = jax.random.randint(jax.random.fold_in(key, 707), (), 9, 17).astype(jnp.int32)
    second_stride = jnp.clip(second_raw, 2, (NK // 2 - 1) // first_stride)
    plane_stride = first_stride * second_stride
    stencil = jnp.stack([jnp.int32(1), jnp.int32(-1), first_stride, -first_stride, plane_stride, -plane_stride]).astype(jnp.int32)
    noise_a = jax.random.randint(jax.random.fold_in(key, 202), (NK, 6), 0, 65536)
    order_ids = jnp.argsort(noise_a * 6 + jnp.arange(6, dtype=jnp.int32)[None, :], axis=-1)[:, :SA - 1]
    fine_ids = jnp.arange(NK, dtype=jnp.int32)
    others = jnp.mod(fine_ids[:, None] + stencil[order_ids], NK)
    a_columns = jnp.concatenate([fine_ids[:, None], others], axis=1).astype(jnp.int32)
    base_counts = jax.random.randint(jax.random.fold_in(key, 303), (NCB,), CAP // 2, CAP + 1)
    full_at = jax.random.randint(jax.random.fold_in(key, 404), (N_ROWS,), 0, RB_DEV)
    is_full = jnp.arange(NCB, dtype=jnp.int32) % RB_DEV == jnp.repeat(full_at, RB_DEV)
    counts = jnp.where(is_full, CAP, base_counts).astype(jnp.int32)
    product_columns = a_columns[r_columns]
    slot_ids = jnp.arange(SR, dtype=jnp.int32)
    favoured = ((slot_ids // SR_DEV)[None, :] == (jnp.arange(NCB, dtype=jnp.int32) % N_INNER)[:, None]) & (slot_ids % SR_DEV < 2)[None, :]
    favoured = favoured[:, :, None] & (jnp.arange(SA, dtype=jnp.int32) == 0)[None, None, :]
    noise_c = jax.random.randint(jax.random.fold_in(key, 505), (NCB, SR, SA), 0, 4096)
    weights = jnp.where(favoured, 0, noise_c + 1)
    packed = (product_columns * 8192 + weights).reshape(NCB, SR * SA)
    ordered = jnp.sort(packed, axis=-1)
    values = ordered // 8192
    ranks = ordered % 8192
    leading = jnp.concatenate([jnp.ones((NCB, 1), dtype=bool), values[:, 1:] != values[:, :-1]], axis=1)
    select_key = jnp.where(leading, ranks * (SR * SA) + jnp.arange(SR * SA, dtype=jnp.int32)[None, :], 2 ** 30)
    selected = jnp.argsort(select_key, axis=-1)[:, :CAP]
    taken = jnp.take_along_axis(values, selected, axis=1)
    c_columns = jnp.where(jnp.arange(CAP, dtype=jnp.int32)[None, :] < counts[:, None], taken, -1).astype(jnp.int32)
    return (r_columns, a_columns, c_columns, counts)


def draw_r_cols(key, part):
    return pattern(key)[0]


def draw_a_cols(key, part):
    return pattern(key)[1]


def draw_c_cols(key, part):
    return pattern(key)[2]


def draw_c_counts(key, part):
    return pattern(key)[3]


def block_levels(own_key, dims, split, smallest, top_value):
    factor_of = 1.0
    for position, parts in split:
        steps = jax.random.uniform(jax.random.fold_in(jax.random.fold_in(own_key, 6), position), (parts,), jnp.float32, smallest / len(split), top_value / len(split))
        factor_of = factor_of * jnp.repeat(jnp.exp(steps), dims[position] // parts).reshape((-1,) + (1,) * (len(dims) - 1 - position))
    return factor_of


def scatter_about(rng, dims, spread, most, split=(), kind=jnp.bfloat16):
    loudness = block_levels(rng, dims, split, -0.22, 0.18) if split else 1.0
    drawn = jax.random.normal(rng, dims, jnp.float32) * spread * loudness
    return jnp.minimum(jnp.maximum(drawn, -most), most).astype(kind)


def setup_inputs(seed: int = 0) -> dict:
    streams_of = jax.random.split(jax.random.key(seed), 7)
    r_tiles = scatter_about(streams_of[0], (NCB, SR, TB, TB), TB ** -0.5, 0.5, ((0, 64), (1, 8)))
    r_cols = draw_r_cols(jax.random.fold_in(streams_of[6], 71), 0)
    a_tiles = scatter_about(streams_of[2], (NK, SA, TB, TB), 1.0, 6.0, ((0, 512),))
    a_cols = draw_a_cols(jax.random.fold_in(streams_of[6], 71), 0)
    c_cols = draw_c_cols(jax.random.fold_in(streams_of[6], 71), 0)
    c_counts = draw_c_counts(jax.random.fold_in(streams_of[6], 71), 0)
    return dict(r_tiles=r_tiles, r_cols=r_cols, a_tiles=a_tiles, a_cols=a_cols, c_cols=c_cols, c_counts=c_counts)


def reference(r_tiles, r_cols, a_tiles, a_cols, c_cols, c_counts):
    def one_row(row_data):
        row_tiles, columns, wanted = row_data
        picked = a_tiles[columns].astype(jnp.float32)
        products = jnp.einsum("jxy,jtyz->jtxz", row_tiles.astype(jnp.float32), picked, precision=lax.Precision.HIGHEST)
        matches = (wanted[:, None, None] == a_cols[columns][None]).astype(jnp.float32)
        summed = jnp.einsum("sjt,jtxz->sxz", matches, products, precision=lax.Precision.HIGHEST)
        return summed.astype(jnp.bfloat16)

    c_tiles = lax.map(one_row, (r_tiles, r_cols, c_cols))
    row_offsets = (jnp.cumsum(c_counts) - c_counts).astype(jnp.int32)
    return c_tiles, row_offsets
```

```python
import functools

import jax
import jax.numpy as jnp
from jax import lax
from jax.experimental import pallas as pl
from jax.experimental.pallas import tpu as pltpu
from jax.sharding import Mesh
from jax.sharding import PartitionSpec as P

I32 = jnp.int32
F32 = jnp.float32
BF16 = jnp.bfloat16
ROWS = ("r0", "r1")
INNER = ("x", "core")
EVERY = ROWS + INNER
FIRST = ("r0", "core")
SECOND = ("r1", "x")
LANES = 128
PACK = 20
STEPS = 256.0
TOP = 32766.0
UNROLL = 4
HEAD = 8


def slot_words(r_ref, c_ref, kinds, keys, count):
    for c in range(count):
        used = jnp.zeros_like(keys)
        fed = jnp.zeros_like(keys)
        for n in range(count):
            used = jnp.where(keys == r_ref[c, n], n + 1, used)
            fed = jnp.where(kinds == c_ref[c, n], n + 1, fed)
        yield c, used, fed


def plan_kernel(wants_ref, win_ref, list_ref, words, table, sem, *, fine, groups, blocks):
    slots = win_ref.shape[1]
    rows = wants_ref.shape[1]
    row = lax.axis_index(ROWS)
    group = lax.axis_index(INNER)
    lane = lax.broadcasted_iota(I32, (slots, LANES), 1)
    half = rows // 2
    for src in range(3):
        first = (row - 1 + src) * (groups * fine) + group * fine
        block = jnp.clip(lax.div(first + LANES, LANES) - 1, 0, blocks - 1)
        keys = block * LANES + lane
        own = (keys >= first) & (keys < first + fine)
        packed = [jnp.zeros((slots, LANES), I32), jnp.zeros((slots, LANES), I32)]
        for c, used, fed in slot_words(wants_ref.at[0], wants_ref.at[1], win_ref[src], keys, rows):
            code = jnp.where(own & (used > 0) & (fed > 0), (fed - 1) * rows + used, 0)
            packed[c // half] = packed[c // half] | (code << (7 * (c % half)))
        words[src, 0, :slots] = packed[0]
        words[src, 1, :slots] = packed[1]
        slot = lax.broadcasted_iota(I32, (slots, LANES), 0)
        marks = jnp.where((packed[0] | packed[1]) != 0, jnp.left_shift(1, slot), 0)
        words[src, 0, slots : slots + 1] = jnp.sum(marks, axis=0, keepdims=True)
    copy = pltpu.make_async_copy(words, table, sem)
    copy.start()
    copy.wait()

    n = jnp.int32(HEAD)
    for src in range(3):
        first = (row - 1 + src) * (groups * fine) + group * fine
        base = lax.rem(first + LANES, LANES)
        began = n

        def fine_row(q, carry, src=src, base=base):
            n, place = carry
            mark = table[src, 0, slots, base + q]

            def found(n, place):
                for t in range(slots):

                    def pairs(n, place, t=t):
                        spot = q * slots + t if src == 1 else place
                        low = table[src, 0, t, base + q]
                        high = table[src, 1, t, base + q]
                        for c in range(rows):
                            code = ((low if c < half else high) >> (7 * (c % half))) & 127
                            list_ref[n] = spot * 512 + c * 64 + jnp.maximum(code - 1, 0)
                            n = n + (code > 0).astype(I32)
                        return n, place + 1

                    n, place = lax.cond((mark & (1 << t)) != 0, pairs, lambda n, place: (n, place), n, place)
                return n, place

            return lax.cond(mark != 0, found, lambda n, place: (n, place), n, place)

        n, _ = lax.fori_loop(0, fine, fine_row, (n, jnp.int32(0)))
        list_ref[src] = n - began


def pack_kernel(
    round_ref, up_ref, down_ref, counts_ref, win_ref, a_ref, up_out, down_out, told_ref, need, flags, sem, copy_sem, *, fine, groups, blocks
):
    slots = win_ref.shape[0]
    rows = up_ref.shape[1]
    pack = up_out.shape[0]
    row = lax.axis_index(ROWS)
    group = lax.axis_index(INNER)
    first = row * (groups * fine) + group * fine
    base = lax.rem(first, LANES)
    lane = lax.broadcasted_iota(I32, (slots, LANES), 1)
    keys = first - base + lane
    own = (keys >= first) & (keys < first + fine)
    for side, ref in enumerate((up_ref, down_ref)):
        wanted = jnp.zeros((slots, LANES), I32)
        for _, used, fed in slot_words(ref.at[0], ref.at[1], win_ref[...], keys, rows):
            wanted = jnp.where(own & (used > 0) & (fed > 0), 1, wanted)
        need[side, :slots] = wanted
    copy = pltpu.make_async_copy(need, flags, sem)
    copy.start()
    copy.wait()
    start = round_ref[0] * pack
    outs = (up_out, down_out)

    def fine_row(q, carry):
        places = list(carry)
        for t in range(slots):
            for side in range(2):
                flag = flags[side, t, base + q]
                place = places[side] - start

                @pl.when((flag > 0) & (place >= 0) & (place < pack))
                def _(side=side, t=t, place=place):
                    pltpu.make_async_copy(a_ref.at[q, t], outs[side].at[place], copy_sem).start()

                places[side] = places[side] + flag
        return tuple(places)

    up_count, down_count = lax.fori_loop(0, fine, fine_row, (jnp.int32(0), jnp.int32(0)))
    sent = jnp.clip(up_count - start, 0, pack) + jnp.clip(down_count - start, 0, pack)

    @pl.loop(0, sent)
    def _(i):
        pltpu.make_async_copy(a_ref.at[0, 0], up_out.at[0], copy_sem).wait()

    total = counts_ref[0]
    for c in range(1, rows):
        total = total + counts_ref[c]
    lane = lax.broadcasted_iota(I32, (1, LANES), 1)
    mine = jnp.where((lane == row) & (group == 0), total, 0)
    over = jnp.maximum(up_count, down_count) > (lane - (blocks - 1)) * pack
    words = mine + jnp.where((lane >= blocks) & over, 1, 0)
    for i in range(told_ref.shape[0]):
        told_ref[i] = words


def product_kernel(round_ref, list_ref, r_ref, own_ref, low_ref, high_ref, *rest, fresh):
    keep_ref, send_ref = rest[-2:]
    pack = low_ref.shape[0]
    cells = keep_ref.shape[0] - 1
    rows = r_ref.shape[0]
    core = lax.axis_index("core")

    @pl.loop(0, cells)
    def _(i):
        for out, old in zip(rest[-2:], rest[:-2] if not fresh else (None, None)):
            out[i] = jnp.zeros(out.shape[1:], F32) if fresh else old[i]

    start = round_ref[0] * pack
    begin = jnp.int32(HEAD)
    for src, ref in enumerate((low_ref, own_ref, high_ref)):
        end = begin + list_ref[src]
        if src == 1 and not fresh:
            begin = end
            continue

        @pl.loop(0, lax.div(end - begin + UNROLL - 1, UNROLL))
        def _(i, src=src, ref=ref, begin=begin, end=end):
            for u in range(UNROLL):
                at = begin + i * UNROLL + u
                entry = list_ref[at]
                place = lax.shift_right_logical(entry, 9)
                row = lax.shift_right_logical(entry, 6) & 7
                slot = lax.shift_right_logical(entry, 3) & 7
                live = at < end
                if src != 1:
                    place = place - start
                    live = live & (place >= 0) & (place < pack)
                place = jnp.where(live, place, 0)
                cell = lax.shift_right_logical(slot, 1) * rows + (row & 7)
                kept = (slot & 1) == core
                part = jnp.dot(r_ref[row & 7, entry & 7], ref[place], preferred_element_type=F32)
                mine = jnp.where(live & kept, cell, cells)
                theirs = jnp.where(live & jnp.logical_not(kept), cell, cells)
                keep_ref[mine] = keep_ref[mine] + part
                send_ref[theirs] = send_ref[theirs] + part

        begin = end


def code_kernel(x_ref, keep_ref, got_ref, own_out, *outs):
    rows, size = own_out.shape[:2]
    step = pl.program_id(0)

    @pl.when(step == len(outs))
    def _():
        own_out[...] = keep_ref[...] + got_ref[...]

    for d, out in enumerate(outs):

        @pl.when(step == d)
        def _(out=out):
            levels = []
            for c in range(rows):
                value = keep_ref[c] + got_ref[c]
                top = jnp.max(jnp.abs(value), axis=0, keepdims=True)
                level = jnp.ceil(jnp.log2(jnp.maximum(top, 1e-30)) * STEPS) + 1.0
                code = jnp.round(value * (jnp.exp2(level * (-1.0 / STEPS)) * TOP))
                out[pl.ds(c * size, size)] = code.astype(I32).astype(jnp.int16)
                levels.append(level)
            levels = jnp.concatenate(levels + levels, axis=0)
            out[pl.ds(rows * size, 2 * rows)] = levels.astype(I32).astype(jnp.int16)


def decode_kernel(own_ref, *refs):
    parts, out_ref = refs[:-1], refs[-1]
    rows = out_ref.shape[0]
    size = out_ref.shape[2]
    scales = [jnp.exp2(p[pl.ds(rows * size, 2 * rows)].astype(F32) * (1.0 / STEPS)) * (1.0 / TOP) for p in parts]
    for c in range(rows):
        total = own_ref[c]
        for p, scale in zip(parts, scales):
            total = total + p[pl.ds(c * size, size)].astype(F32) * scale[c : c + 1]
        out_ref[c, 0] = total.astype(BF16)


def offset_kernel(counts_ref, parts_ref, out_ref, turns_ref, *, blocks):
    row = lax.axis_index(ROWS)
    words = parts_ref[0]
    for i in range(1, parts_ref.shape[0]):
        words = words + parts_ref[i]
    lane = lax.broadcasted_iota(I32, words.shape, 1)
    turns_ref[0] = 1 + jnp.sum(((lane >= blocks) & (words > 0)).astype(I32))
    offset = jnp.sum(jnp.where(lane < row, words, 0))
    for c in range(out_ref.shape[0]):
        out_ref[c] = offset
        offset = offset + counts_ref[c]


def smem():
    return pl.BlockSpec(memory_space=pltpu.SMEM)


def vmem():
    return pl.BlockSpec(memory_space=pltpu.VMEM)


def anywhere():
    return pl.BlockSpec(memory_space=pl.ANY)


def shape(dims, dtype):
    return jax.ShapeDtypeStruct(dims, dtype)


def told(parts, axes):
    return jnp.sum(lax.all_to_all(parts, axes, 0, 0, tiled=True), axis=(0, 1))


def body(r_tiles, r_cols, a_tiles, a_cols, c_cols, c_counts):
    fine, op_slots, size, _ = a_tiles.shape
    rows, r_slots = r_tiles.shape[:2]
    groups = lax.axis_size(INNER)
    chips = lax.axis_size("x")
    row_blocks = lax.axis_size(ROWS)
    row = lax.axis_index(ROWS)
    group = lax.axis_index(INNER)
    blocks = a_cols.shape[0] // LANES
    pack = PACK
    cap = c_cols.shape[1]
    limit = lambda mb: pltpu.CompilerParams(vmem_limit_bytes=mb * 2**20)

    to_next = [(i, i + 1) for i in range(row_blocks - 1)]
    to_last = [(i + 1, i) for i in range(row_blocks - 1)]

    wants = jnp.stack([r_cols, c_cols])
    above = lax.ppermute(wants, ROWS, to_last)
    below = lax.ppermute(wants, ROWS, to_next)

    by_slot = a_cols.T

    def window(block_row):
        first = block_row * (groups * fine) + group * fine
        block = jnp.clip((first + LANES) // LANES - 1, 0, blocks - 1)
        return lax.dynamic_slice(by_slot, (0, block * LANES), (op_slots, LANES))

    own_window = window(row)
    windows = jnp.stack([window(row - 1), own_window, window(row + 1)])
    pairs = pl.pallas_call(
        functools.partial(plan_kernel, fine=fine, groups=groups, blocks=blocks),
        in_specs=[smem(), vmem()],
        out_specs=smem(),
        out_shape=shape((rows * r_slots * op_slots + 64,), I32),
        scratch_shapes=[
            pltpu.VMEM((3, 2, 8, LANES), I32),
            pltpu.SMEM((3, 2, 8, LANES), I32),
            pltpu.SemaphoreType.DMA,
        ],
        compiler_params=limit(4),
        name="plan",
    )(wants, windows)

    own_tiles = a_tiles.reshape(fine * op_slots, size, size)

    firsts, seconds = lax.axis_size(FIRST), lax.axis_size(SECOND)

    def exchange(turn):
        up, down, words = pl.pallas_call(
            functools.partial(pack_kernel, fine=fine, groups=groups, blocks=row_blocks),
            in_specs=[smem(), smem(), smem(), smem(), vmem(), anywhere()],
            out_specs=[anywhere(), anywhere(), vmem()],
            out_shape=[
                shape((pack, size, size), BF16),
                shape((pack, size, size), BF16),
                shape((firsts, 1, LANES), I32),
            ],
            scratch_shapes=[
                pltpu.VMEM((2, 8, LANES), I32),
                pltpu.SMEM((2, 8, LANES), I32),
                pltpu.SemaphoreType.DMA,
                pltpu.SemaphoreType.DMA,
            ],
            compiler_params=limit(4),
            name="pack",
        )(turn, above, below, c_counts, own_window, a_tiles)
        low = lax.ppermute(up, ROWS, to_next)
        high = lax.ppermute(down, ROWS, to_last)
        return low, high, words

    half = (chips * rows + 1, size, size)

    def product(turn, low, high, sums):
        fresh = sums is None
        return pl.pallas_call(
            functools.partial(product_kernel, fresh=fresh),
            in_specs=[smem(), smem()] + [vmem()] * (4 if fresh else 6),
            out_specs=[vmem(), vmem()],
            out_shape=[shape(half, F32)] * 2,
            compiler_params=limit(20),
            name="products" if fresh else "more_products",
        )(turn, pairs, r_tiles, own_tiles, low, high, *(() if fresh else sums))

    coded_rows = rows * size + 2 * rows
    chip = lax.axis_index("x")[None]
    others = range(1, chips)

    def chunk(i, x):
        return (lax.rem(x[0] + i + 1, chips), 0, 0)

    def coded(keep, send):
        got = lax.ppermute(send, "core", [(0, 1), (1, 0)])
        return pl.pallas_call(
            code_kernel,
            grid_spec=pltpu.PrefetchScalarGridSpec(
                num_scalar_prefetch=1,
                grid=(chips,),
                in_specs=[pl.BlockSpec((rows, size, size), chunk)] * 2,
                out_specs=[pl.BlockSpec((rows, size, size), lambda i, x: (0, 0, 0))]
                + [pl.BlockSpec((coded_rows, size), lambda i, x: (0, 0))] * len(others),
            ),
            out_shape=[shape((rows, size, size), F32)] + [shape((coded_rows, size), jnp.int16)] * len(others),
            compiler_params=limit(20),
            name="code",
        )(chip, keep, got)

    def swapped(codes):
        return [lax.ppermute(code, "x", [(i, (i + d) % chips) for i in range(chips)]) for d, code in zip(others, codes)]

    def finish(own, parts):
        return pl.pallas_call(
            decode_kernel,
            in_specs=[vmem()] * chips,
            out_specs=vmem(),
            out_shape=shape((rows, 1, size, size), BF16),
            compiler_params=limit(16),
            name="decode",
        )(own, *parts)

    low, high, words = exchange(jnp.zeros((1,), I32))
    shared = told(words, FIRST)
    turn, shared = lax.optimization_barrier((jnp.zeros((1,), I32), shared))
    keep, send = product(turn, low, high, None)
    own, *codes = coded(keep, send)
    parts = swapped(codes)
    shared = jnp.broadcast_to(shared[None, None], (seconds, 1, LANES))
    shared = lax.all_to_all(shared, SECOND, 0, 0, tiled=True)
    c_tiles = finish(own, parts)
    row_offsets, turns = pl.pallas_call(
        functools.partial(offset_kernel, blocks=row_blocks),
        in_specs=[smem(), vmem()],
        out_specs=[smem(), smem()],
        out_shape=[shape((rows,), I32), shape((1,), I32)],
        compiler_params=limit(4),
        name="offsets",
    )(c_counts, shared)

    def more(state):
        turn, keep, send, _ = state
        low, high, _ = exchange(turn[None])
        keep, send = product(turn[None], low, high, (keep, send))
        own, *codes = coded(keep, send)
        return turn + 1, keep, send, finish(own, swapped(codes))

    state = (jnp.int32(1), keep, send, c_tiles)
    c_tiles = lax.while_loop(lambda state: state[0] < turns[0], more, state)[3]
    return (c_tiles, row_offsets)


def solution(mesh):
    finer = Mesh(mesh.devices.reshape(8, mesh.shape["rows"] // 8, mesh.shape["inner"] // 2, 2), EVERY)
    return jax.shard_map(
        body,
        mesh=finer,
        in_specs=(
            P(ROWS, INNER, None, None),
            P(ROWS, INNER),
            P(EVERY, None, None, None),
            P(),
            P(ROWS, None),
            P(ROWS),
        ),
        out_specs=(P(ROWS, INNER, None, None), P(ROWS)),
        check_vma=False,
    )
```

```python
import functools

import jax
import jax.numpy as jnp
from jax import lax
from jax.experimental import pallas as pl
from jax.experimental.pallas import tpu as pltpu
from jax.sharding import Mesh
from jax.sharding import PartitionSpec as P


I32 = jnp.int32
F32 = jnp.float32
BF16 = jnp.bfloat16
ROWS = ("r0", "r1")
INNER = ("x", "core")
EVERY = ROWS + INNER
FIRST = ("r0", "x", "core")
SECOND = "r1"
LANES = 128
PACK = 20
STEPS = 256.0
TOP = 32766.0
UNROLL = 4
HEAD = 8


def slot_words(r_ref, c_ref, kinds, keys, count):
    for c in range(count):
        used = jnp.zeros_like(keys)
        fed = jnp.zeros_like(keys)
        for n in range(count):
            used = jnp.where(keys == r_ref[c, n], n + 1, used)
            fed = jnp.where(kinds == c_ref[c, n], n + 1, fed)
        yield c, used, fed


def plan_kernel(wants_ref, win_ref, list_ref, words, table, sem, *, fine, groups, blocks):
    slots = win_ref.shape[1]
    rows = wants_ref.shape[1]
    row = lax.axis_index(ROWS)
    group = lax.axis_index(INNER)
    lane = lax.broadcasted_iota(I32, (slots, LANES), 1)
    half = rows // 2
    for src in range(3):
        first = (row - 1 + src) * (groups * fine) + group * fine
        block = jnp.clip(lax.div(first + LANES, LANES) - 1, 0, blocks - 1)
        keys = block * LANES + lane
        own = (keys >= first) & (keys < first + fine)
        packed = [jnp.zeros((slots, LANES), I32), jnp.zeros((slots, LANES), I32)]
        for c, used, fed in slot_words(wants_ref.at[0], wants_ref.at[1], win_ref[src], keys, rows):
            code = jnp.where(own & (used > 0) & (fed > 0), (fed - 1) * rows + used, 0)
            packed[c // half] = packed[c // half] | (code << (7 * (c % half)))
        words[src, 0, :slots] = packed[0]
        words[src, 1, :slots] = packed[1]
        slot = lax.broadcasted_iota(I32, (slots, LANES), 0)
        marks = jnp.where((packed[0] | packed[1]) != 0, jnp.left_shift(1, slot), 0)
        words[src, 0, slots : slots + 1] = jnp.sum(marks, axis=0, keepdims=True)
    copy = pltpu.make_async_copy(words, table, sem)
    copy.start()
    copy.wait()

    n = jnp.int32(HEAD)
    for src in range(3):
        first = (row - 1 + src) * (groups * fine) + group * fine
        base = lax.rem(first + LANES, LANES)
        began = n

        def fine_row(q, carry, src=src, base=base):
            n, place = carry
            mark = table[src, 0, slots, base + q]

            def found(n, place):
                for t in range(slots):

                    def pairs(n, place, t=t):
                        spot = (q * slots + t) * 64 + place
                        low = table[src, 0, t, base + q]
                        high = table[src, 1, t, base + q]
                        for c in range(rows):
                            code = ((low if c < half else high) >> (7 * (c % half))) & 127
                            list_ref[n] = spot * 512 + c * 64 + jnp.maximum(code - 1, 0)
                            n = n + (code > 0).astype(I32)
                        return n, place + 1

                    n, place = lax.cond((mark & (1 << t)) != 0, pairs, lambda n, place: (n, place), n, place)
                return n, place

            return lax.cond(mark != 0, found, lambda n, place: (n, place), n, place)

        n, _ = lax.fori_loop(0, fine, fine_row, (n, jnp.int32(0)))
        list_ref[src] = n - began


def pack_kernel(
    up_ref, down_ref, counts_ref, win_ref, a_ref, up_out, down_out, told_ref, need, flags, counts, sem, count_sem, copy_sem, *, fine, groups, blocks
):
    slots = win_ref.shape[0]
    rows = up_ref.shape[1]
    pack = up_out.shape[0]
    load = pltpu.make_async_copy(counts_ref, counts, count_sem)
    load.start()
    row = lax.axis_index(ROWS)
    group = lax.axis_index(INNER)
    first = row * (groups * fine) + group * fine
    base = lax.rem(first, LANES)
    lane = lax.broadcasted_iota(I32, (slots, LANES), 1)
    slot = lax.broadcasted_iota(I32, (slots, LANES), 0)
    keys = first - base + lane
    own = (keys >= first) & (keys < first + fine)
    for side, ref in enumerate((up_ref, down_ref)):
        wanted = jnp.zeros((slots, LANES), I32)
        for _, used, fed in slot_words(ref.at[0], ref.at[1], win_ref[...], keys, rows):
            wanted = jnp.where(own & (used > 0) & (fed > 0), jnp.left_shift(1, slot), wanted)
        need[side : side + 1] = jnp.sum(wanted, axis=0, keepdims=True)
    copy = pltpu.make_async_copy(need, flags, sem)
    copy.start()
    copy.wait()
    outs = (up_out, down_out)

    def fine_row(q, places):
        after = []
        for side in range(2):
            mark = flags[side, base + q]
            place = places[side]

            def found(place, side=side, mark=mark):
                for t in range(slots):
                    flag = lax.shift_right_logical(mark, t) & 1

                    @pl.when((flag > 0) & (place < pack))
                    def _(t=t, place=place):
                        pltpu.make_async_copy(a_ref.at[q, t], outs[side].at[place], copy_sem).start()

                    place = place + flag
                return place

            after.append(lax.cond(mark != 0, found, lambda place: place, place))
        return tuple(after)

    up_count, down_count = lax.fori_loop(0, fine, fine_row, (jnp.int32(0), jnp.int32(0)))

    load.wait()
    total = counts[0]
    for c in range(1, rows):
        total = total + counts[c]
    lane = lax.broadcasted_iota(I32, (1, LANES), 1)
    mine = jnp.where((lane == row) & (group == 0), total, 0)
    over = (jnp.maximum(up_count, down_count) > pack).astype(I32)
    words = jnp.where(lane == blocks, over, mine)
    for i in range(told_ref.shape[0]):
        told_ref[i] = words

    @pl.loop(0, jnp.minimum(up_count, pack) + jnp.minimum(down_count, pack))
    def _(i):
        pltpu.make_async_copy(a_ref.at[0, 0], up_out.at[0], copy_sem).wait()


def product_kernel(list_ref, r_ref, own_ref, low_ref, high_ref, keep_ref, send_ref, *, whole):
    pack = low_ref.shape[0]
    cells = keep_ref.shape[0] - 1
    rows = r_ref.shape[0]
    core = lax.axis_index("core")

    @pl.loop(0, cells)
    def _(i):
        keep_ref[i] = jnp.zeros(keep_ref.shape[1:], F32)
        send_ref[i] = jnp.zeros(send_ref.shape[1:], F32)

    begin = jnp.int32(HEAD)
    for src, ref in enumerate((low_ref, own_ref, high_ref)):
        end = begin + list_ref[src]

        @pl.loop(0, lax.div(end - begin + UNROLL - 1, UNROLL))
        def _(i, src=src, ref=ref, begin=begin, end=end):
            for u in range(UNROLL):
                at = begin + i * UNROLL + u
                entry = list_ref[at]
                spot = lax.shift_right_logical(entry, 15) & 63
                place = lax.shift_right_logical(entry, 9) & 63
                row = lax.shift_right_logical(entry, 6) & 7
                slot = lax.shift_right_logical(entry, 3) & 7
                live = at < end
                if src == 1 or whole:
                    place = spot
                else:
                    live = live & (place < pack)
                place = jnp.where(live, place, 0)
                cell = lax.shift_right_logical(slot, 1) * rows + row
                kept = (slot & 1) == core
                part = jnp.dot(r_ref[row, entry & 7], ref[place], preferred_element_type=F32)
                mine = jnp.where(live & kept, cell, cells)
                theirs = jnp.where(live & jnp.logical_not(kept), cell, cells)
                keep_ref[mine] = keep_ref[mine] + part
                send_ref[theirs] = send_ref[theirs] + part

        begin = end


def code_kernel(keep_ref, got_ref, own_out, out):
    rows, size = own_out.shape[:2]
    here = pl.program_id(0) == lax.axis_index("x")

    @pl.when(here)
    def _():
        own_out[...] = keep_ref[...] + got_ref[...]

    @pl.when(jnp.logical_not(here))
    def _():
        levels = []
        for c in range(rows):
            value = keep_ref[c] + got_ref[c]
            top = jnp.max(jnp.abs(value), axis=0, keepdims=True)
            level = jnp.ceil(jnp.log2(jnp.maximum(top, 1e-30)) * STEPS) + 1.0
            code = jnp.round(value * (jnp.exp2(level * (-1.0 / STEPS)) * TOP))
            out[0, pl.ds(c * size, size)] = code.astype(I32).astype(jnp.int16)
            levels.append(level)
        levels = jnp.concatenate(levels + levels, axis=0)
        out[0, pl.ds(rows * size, 2 * rows)] = levels.astype(I32).astype(jnp.int16)


def decode_kernel(own_ref, code_ref, out_ref):
    rows = out_ref.shape[0]
    size = out_ref.shape[2]
    chip = lax.axis_index("x")
    parts = range(code_ref.shape[0])
    scales = [
        jnp.exp2(code_ref[p, pl.ds(rows * size, 2 * rows)].astype(F32) * (1.0 / STEPS)) * (1.0 / TOP) for p in parts
    ]
    for c in range(rows):
        total = own_ref[c]
        for p in parts:
            value = code_ref[p, pl.ds(c * size, size)].astype(F32) * scales[p][c : c + 1]
            total = total + jnp.where(p == chip, 0.0, value)
        out_ref[c, 0] = total.astype(BF16)


def offset_kernel(counts_ref, parts_ref, out_ref, over_ref, *, blocks):
    row = lax.axis_index(ROWS)
    words = parts_ref[...]
    lane = lax.broadcasted_iota(I32, words.shape, 1)
    over_ref[0] = jnp.sum(jnp.where(lane == blocks, words, 0))
    offset = jnp.sum(jnp.where(lane < row, words, 0))
    for c in range(out_ref.shape[0]):
        out_ref[c] = offset
        offset = offset + counts_ref[c]


def smem():
    return pl.BlockSpec(memory_space=pltpu.SMEM)


def vmem():
    return pl.BlockSpec(memory_space=pltpu.VMEM)


def anywhere():
    return pl.BlockSpec(memory_space=pl.ANY)


def shape(dims, dtype):
    return jax.ShapeDtypeStruct(dims, dtype)


def body(r_tiles, r_cols, a_tiles, a_cols, c_cols, c_counts):
    fine, op_slots, size, _ = a_tiles.shape
    rows, r_slots = r_tiles.shape[:2]
    groups = lax.axis_size(INNER)
    chips = lax.axis_size("x")
    row_blocks = lax.axis_size(ROWS)
    row = lax.axis_index(ROWS)
    group = lax.axis_index(INNER)
    blocks = a_cols.shape[0] // LANES
    limit = lambda mb: pltpu.CompilerParams(vmem_limit_bytes=mb * 2**20)

    to_next = [(i, i + 1) for i in range(row_blocks - 1)]
    to_last = [(i + 1, i) for i in range(row_blocks - 1)]

    wants = jnp.stack([r_cols, c_cols])
    below = lax.ppermute(wants, ROWS, to_next)
    above = lax.ppermute(wants, ROWS, to_last)

    by_slot = a_cols.T

    def window(block_row):
        first = block_row * (groups * fine) + group * fine
        block = jnp.clip((first + LANES) // LANES - 1, 0, blocks - 1)
        return lax.dynamic_slice(by_slot, (0, block * LANES), (op_slots, LANES))

    own_window = window(row)
    windows = jnp.stack([window(row - 1), own_window, window(row + 1)])
    firsts = lax.axis_size(FIRST)
    own_tiles = a_tiles.reshape(fine * op_slots, size, size)
    sums = shape((chips * rows + 1, size, size), F32)
    coded_rows = rows * size + 2 * rows

    def plan():
        return pl.pallas_call(
            functools.partial(plan_kernel, fine=fine, groups=groups, blocks=blocks),
            in_specs=[smem(), vmem()],
            out_specs=smem(),
            out_shape=shape((rows * r_slots * op_slots + 64,), I32),
            scratch_shapes=[
                pltpu.VMEM((3, 2, 8, LANES), I32),
                pltpu.SMEM((3, 2, 8, LANES), I32),
                pltpu.SemaphoreType.DMA,
            ],
            compiler_params=limit(4),
            name="plan",
        )(wants, windows)

    def packed():
        return pl.pallas_call(
            functools.partial(pack_kernel, fine=fine, groups=groups, blocks=row_blocks),
            in_specs=[smem(), smem(), anywhere(), vmem(), anywhere()],
            out_specs=[anywhere(), anywhere(), vmem()],
            out_shape=[
                shape((PACK, size, size), BF16),
                shape((PACK, size, size), BF16),
                shape((firsts, 1, LANES), I32),
            ],
            scratch_shapes=[
                pltpu.VMEM((8, LANES), I32),
                pltpu.SMEM((8, LANES), I32),
                pltpu.SMEM((rows,), I32),
                pltpu.SemaphoreType.DMA,
                pltpu.SemaphoreType.DMA,
                pltpu.SemaphoreType.DMA,
            ],
            compiler_params=limit(4),
            name="pack",
        )(above, below, c_counts, own_window, a_tiles)

    def product(low, high, whole):
        return pl.pallas_call(
            functools.partial(product_kernel, whole=whole),
            in_specs=[smem()] + [vmem()] * 4,
            out_specs=[vmem(), vmem()],
            out_shape=[sums, sums],
            compiler_params=limit(20),
            name="all_products" if whole else "products",
        )(pairs, r_tiles, own_tiles, low, high)

    def coded(keep, send):
        got = lax.ppermute(send, "core", [(0, 1), (1, 0)])
        chunk = pl.BlockSpec((rows, size, size), lambda i: (i, 0, 0))
        return pl.pallas_call(
            code_kernel,
            grid=(chips,),
            in_specs=[chunk, chunk],
            out_specs=[
                pl.BlockSpec((rows, size, size), lambda i: (0, 0, 0)),
                pl.BlockSpec((1, coded_rows, size), lambda i: (i, 0, 0)),
            ],
            out_shape=[shape((rows, size, size), F32), shape((chips, coded_rows, size), jnp.int16)],
            compiler_params=limit(20),
            name="code",
        )(keep, got)

    def finish(own, codes):
        return pl.pallas_call(
            decode_kernel,
            in_specs=[vmem(), vmem()],
            out_specs=vmem(),
            out_shape=shape((rows, 1, size, size), BF16),
            compiler_params=limit(16),
            name="decode",
        )(own, codes)

    up, down, words = packed()
    low = lax.ppermute(up, ROWS, to_next)
    high = lax.ppermute(down, ROWS, to_last)
    shared = lax.all_to_all(words, FIRST, 0, 0, tiled=True)
    pairs = plan()
    keep, send = product(low, high, False)
    own, codes = coded(keep, send)
    codes = lax.all_to_all(codes, "x", 0, 0, tiled=True)
    shared = lax.psum(jnp.sum(shared, axis=0), SECOND)
    c_tiles = finish(own, codes)
    row_offsets, over = pl.pallas_call(
        functools.partial(offset_kernel, blocks=row_blocks),
        in_specs=[smem(), vmem()],
        out_specs=[smem(), smem()],
        out_shape=[shape((rows,), I32), shape((1,), I32)],
        compiler_params=limit(4),
        name="offsets",
    )(c_counts, shared)

    def redo(state):
        low = lax.ppermute(own_tiles, ROWS, to_next)
        high = lax.ppermute(own_tiles, ROWS, to_last)
        own, codes = coded(*product(low, high, True))
        return jnp.int32(0), finish(own, lax.all_to_all(codes, "x", 0, 0, tiled=True))

    c_tiles = lax.while_loop(lambda state: state[0] > 0, redo, (over[0], c_tiles))[1]
    return (c_tiles, row_offsets)


def solution(mesh):
    finer = Mesh(mesh.devices.reshape(8, mesh.shape["rows"] // 8, mesh.shape["inner"] // 2, 2), EVERY)
    return jax.shard_map(
        body,
        mesh=finer,
        in_specs=(
            P(ROWS, INNER, None, None),
            P(ROWS, INNER),
            P(EVERY, None, None, None),
            P(),
            P(ROWS, None),
            P(ROWS),
        ),
        out_specs=(P(ROWS, INNER, None, None), P(ROWS)),
        check_vma=False,
    )
```

```python
import functools

import jax
import jax.numpy as jnp
from jax import lax
from jax.experimental import pallas as pl
from jax.experimental.pallas import tpu as pltpu
from jax.sharding import Mesh
from jax.sharding import PartitionSpec as P


I32 = jnp.int32
F32 = jnp.float32
BF16 = jnp.bfloat16
ROWS = ("r0", "r1")
INNER = ("x", "core")
EVERY = ROWS + INNER
FIRST = ("r0", "x", "core")
SECOND = "r1"
LANES = 128
PACK = 20
STEPS = 256.0
TOP = 32766.0
UNROLL = 4
HEAD = 8
HALF = 512


def slot_words(wants_ref, kinds, keys, count):
    for c in range(count):
        used = jnp.zeros_like(keys)
        fed = jnp.zeros_like(keys)
        for n in range(count):
            used = jnp.where(keys == wants_ref[c, n], n + 1, used)
            fed = jnp.where(kinds == wants_ref[count + c, n], n + 1, fed)
        yield c, used, fed


def plan_kernel(
    wants_ref, win_ref, r_ref, a_ref, list_ref, r_out, a_out, words, table, sem, load_sems, *, fine, groups, blocks
):
    loads = [
        pltpu.make_async_copy(r_ref, r_out, load_sems.at[0]),
        pltpu.make_async_copy(a_ref, a_out, load_sems.at[1]),
    ]
    for load in loads:
        load.start()
    slots = win_ref.shape[1]
    rows = wants_ref.shape[1]
    core = lax.axis_index("core")
    row = lax.axis_index(ROWS)
    group = lax.axis_index(INNER)
    lane = lax.broadcasted_iota(I32, (slots, LANES), 1)
    half = rows // 2
    for src in range(3):
        first = (row - 1 + src) * (groups * fine) + group * fine
        block = jnp.clip(lax.div(first + LANES, LANES) - 1, 0, blocks - 1)
        keys = block * LANES + lane
        own = (keys >= first) & (keys < first + fine)
        packed = [jnp.zeros((slots, LANES), I32), jnp.zeros((slots, LANES), I32)]
        for c, used, fed in slot_words(wants_ref, win_ref[src], keys, rows):
            code = jnp.where(own & (used > 0) & (fed > 0), (fed - 1) * rows + used, 0)
            packed[c // half] = packed[c // half] | (code << (7 * (c % half)))
        words[src, 0, :slots] = packed[0]
        words[src, 1, :slots] = packed[1]
        slot = lax.broadcasted_iota(I32, (slots, LANES), 0)
        marks = jnp.where((packed[0] | packed[1]) != 0, jnp.left_shift(1, slot), 0)
        words[src, 0, slots : slots + 1] = jnp.sum(marks, axis=0, keepdims=True)
    copy = pltpu.make_async_copy(words, table, sem)
    copy.start()
    copy.wait()

    n = (jnp.int32(HEAD), jnp.int32(HALF))
    for src in range(3):
        first = (row - 1 + src) * (groups * fine) + group * fine
        base = lax.rem(first + LANES, LANES)
        began = n

        def fine_row(q, carry, src=src, base=base):
            mark = table[src, 0, slots, base + q]

            def found(carry):
                for t in range(slots):

                    def pairs(carry, t=t):
                        sent, kept, place = carry
                        spot = (q * slots + t) * 64 + place
                        low = table[src, 0, t, base + q]
                        high = table[src, 1, t, base + q]
                        for c in range(rows):
                            code = (((low if c < half else high) >> (7 * (c % half))) & 127) - 1
                            mine = ((code >> 3) & 1) == core
                            list_ref[jnp.where(mine, kept, sent)] = spot * 512 + c * 64 + jnp.maximum(code, 0)
                            live = code >= 0
                            kept = kept + (live & mine).astype(I32)
                            sent = sent + (live & jnp.logical_not(mine)).astype(I32)
                        return sent, kept, place + 1

                    carry = lax.cond((mark & (1 << t)) != 0, pairs, lambda carry: carry, carry)
                return carry

            return lax.cond(mark != 0, found, lambda carry: carry, carry)

        n = lax.fori_loop(0, fine, fine_row, (*n, jnp.int32(0)))[:2]
        list_ref[src] = n[0] - began[0]
        list_ref[3 + src] = n[1] - began[1]
    for load in loads:
        load.wait()


def pack_kernel(
    up_ref, down_ref, wants_ref, win_ref, a_ref, up_out, down_out, told_ref, need, flags, sem, copy_sem, *, fine, groups, blocks
):
    slots = win_ref.shape[0]
    rows = up_ref.shape[1]
    pack = up_out.shape[0]
    row = lax.axis_index(ROWS)
    group = lax.axis_index(INNER)
    first = row * (groups * fine) + group * fine
    base = lax.rem(first, LANES)
    lane = lax.broadcasted_iota(I32, (slots, LANES), 1)
    slot = lax.broadcasted_iota(I32, (slots, LANES), 0)
    keys = first - base + lane
    own = (keys >= first) & (keys < first + fine)
    for side, ref in enumerate((up_ref, down_ref)):
        wanted = jnp.zeros((slots, LANES), I32)
        for _, used, fed in slot_words(ref, win_ref[...], keys, rows):
            wanted = jnp.where(own & (used > 0) & (fed > 0), jnp.left_shift(1, slot), wanted)
        need[side : side + 1] = jnp.sum(wanted, axis=0, keepdims=True)
    copy = pltpu.make_async_copy(need, flags, sem)
    copy.start()
    copy.wait()
    outs = (up_out, down_out)

    def fine_row(q, places):
        after = []
        for side in range(2):
            mark = flags[side, base + q]
            place = places[side]

            def found(place, side=side, mark=mark):
                for t in range(slots):
                    flag = lax.shift_right_logical(mark, t) & 1

                    @pl.when((flag > 0) & (place < pack))
                    def _(t=t, place=place):
                        pltpu.make_async_copy(a_ref.at[q, t], outs[side].at[place], copy_sem).start()

                    place = place + flag
                return place

            after.append(lax.cond(mark != 0, found, lambda place: place, place))
        return tuple(after)

    up_count, down_count = lax.fori_loop(0, fine, fine_row, (jnp.int32(0), jnp.int32(0)))

    total = wants_ref[2 * rows, 0]
    for c in range(1, rows):
        total = total + wants_ref[2 * rows, c]
    lane = lax.broadcasted_iota(I32, (1, LANES), 1)
    mine = jnp.where((lane == row) & (group == 0), total, 0)
    over = (jnp.maximum(up_count, down_count) > pack).astype(I32)
    words = jnp.where(lane == blocks, over, mine)
    told_ref[...] = words

    @pl.loop(0, jnp.minimum(up_count, pack) + jnp.minimum(down_count, pack))
    def _(i):
        pltpu.make_async_copy(a_ref.at[0, 0], up_out.at[0], copy_sem).wait()


def product_kernel(list_ref, r_ref, own_ref, low_ref, high_ref, out_ref, *, side, whole):
    pack = low_ref.shape[0]
    cells = out_ref.shape[0] - 1
    rows = r_ref.shape[0]

    @pl.loop(0, cells)
    def _(i):
        out_ref[i] = jnp.zeros(out_ref.shape[1:], F32)

    begin = jnp.int32(HALF if side else HEAD)
    for src, ref in enumerate((low_ref, own_ref, high_ref)):
        end = begin + list_ref[3 * side + src]

        @pl.loop(0, lax.div(end - begin + UNROLL - 1, UNROLL))
        def _(i, src=src, ref=ref, begin=begin, end=end):
            for u in range(UNROLL):
                at = begin + i * UNROLL + u
                entry = list_ref[at]
                spot = lax.shift_right_logical(entry, 15) & 63
                place = lax.shift_right_logical(entry, 9) & 63
                row = lax.shift_right_logical(entry, 6) & 7
                slot = lax.shift_right_logical(entry, 3) & 7
                live = at < end
                if src == 1 or whole:
                    place = spot
                else:
                    live = live & (place < pack)
                place = jnp.where(live, place, 0)
                cell = jnp.where(live, lax.shift_right_logical(slot, 1) * rows + row, cells)
                part = jnp.dot(r_ref[row, entry & 7], ref[place], preferred_element_type=F32)
                out_ref[cell] = out_ref[cell] + part

        begin = end


def code_kernel(keep_ref, got_ref, own_out, out):
    rows, size = own_out.shape[:2]
    here = pl.program_id(0) == lax.axis_index("x")

    @pl.when(here)
    def _():
        own_out[...] = keep_ref[...] + got_ref[...]

    @pl.when(jnp.logical_not(here))
    def _():
        levels = []
        for c in range(rows):
            value = keep_ref[c] + got_ref[c]
            top = jnp.max(jnp.abs(value), axis=0, keepdims=True)
            level = jnp.ceil(jnp.log2(jnp.maximum(top, 1e-30)) * STEPS) + 1.0
            code = jnp.round(value * (jnp.exp2(level * (-1.0 / STEPS)) * TOP))
            out[0, pl.ds(c * size, size)] = code.astype(I32).astype(jnp.int16)
            levels.append(level)
        levels = jnp.concatenate(levels + levels, axis=0)
        out[0, pl.ds(rows * size, 2 * rows)] = levels.astype(I32).astype(jnp.int16)


def decode_kernel(own_ref, code_ref, out_ref):
    rows = out_ref.shape[0]
    size = out_ref.shape[2]
    chip = lax.axis_index("x")
    parts = range(code_ref.shape[0])
    scales = [
        jnp.exp2(code_ref[p, pl.ds(rows * size, 2 * rows)].astype(F32) * (1.0 / STEPS)) * (1.0 / TOP) for p in parts
    ]
    for c in range(rows):
        total = own_ref[c]
        for p in parts:
            value = code_ref[p, pl.ds(c * size, size)].astype(F32) * scales[p][c : c + 1]
            total = total + jnp.where(p == chip, 0.0, value)
        out_ref[c, 0] = total.astype(BF16)


def offset_kernel(counts_ref, parts_ref, out_ref, over_ref, *, blocks):
    row = lax.axis_index(ROWS)
    words = parts_ref[...]
    lane = lax.broadcasted_iota(I32, words.shape, 1)
    over_ref[0] = jnp.sum(jnp.where(lane == blocks, words, 0))
    offset = jnp.sum(jnp.where(lane < row, words, 0))
    for c in range(out_ref.shape[0]):
        out_ref[c] = offset
        offset = offset + counts_ref[c]


def smem():
    return pl.BlockSpec(memory_space=pltpu.SMEM)


def vmem():
    return pl.BlockSpec(memory_space=pltpu.VMEM)


def anywhere():
    return pl.BlockSpec(memory_space=pl.ANY)


def shape(dims, dtype):
    return jax.ShapeDtypeStruct(dims, dtype)


def body(r_tiles, r_cols, a_tiles, a_cols, c_cols, c_counts):
    fine, op_slots, size, _ = a_tiles.shape
    rows, _ = r_tiles.shape[:2]
    groups = lax.axis_size(INNER)
    chips = lax.axis_size("x")
    row_blocks = lax.axis_size(ROWS)
    row = lax.axis_index(ROWS)
    group = lax.axis_index(INNER)
    blocks = a_cols.shape[0] // LANES
    limit = lambda mb: pltpu.CompilerParams(vmem_limit_bytes=mb * 2**20)

    to_next = [(i, i + 1) for i in range(row_blocks - 1)]
    to_last = [(i + 1, i) for i in range(row_blocks - 1)]

    wants = jnp.concatenate([r_cols, c_cols, c_counts[None]])
    below = lax.ppermute(wants, ROWS, to_next)
    above = lax.ppermute(wants, ROWS, to_last)

    by_slot = a_cols.T

    def window(block_row):
        first = block_row * (groups * fine) + group * fine
        block = jnp.clip((first + LANES) // LANES - 1, 0, blocks - 1)
        return lax.dynamic_slice(by_slot, (0, block * LANES), (op_slots, LANES))

    own_window = window(row)
    windows = jnp.stack([window(row - 1), own_window, window(row + 1)])
    firsts = lax.axis_size(FIRST)
    own_tiles = a_tiles.reshape(fine * op_slots, size, size)
    sums = shape((chips * rows + 1, size, size), F32)
    coded_rows = rows * size + 2 * rows

    def plan():
        return pl.pallas_call(
            functools.partial(plan_kernel, fine=fine, groups=groups, blocks=blocks),
            in_specs=[smem(), vmem(), anywhere(), anywhere()],
            out_specs=[smem(), vmem(), vmem()],
            out_shape=[
                shape((2 * HALF,), I32),
                pltpu.VMEM(r_tiles.shape, BF16),
                pltpu.VMEM(own_tiles.shape, BF16),
            ],
            scratch_shapes=[
                pltpu.VMEM((3, 2, 8, LANES), I32),
                pltpu.SMEM((3, 2, 8, LANES), I32),
                pltpu.SemaphoreType.DMA,
                pltpu.SemaphoreType.DMA((2,)),
            ],
            compiler_params=limit(8),
            name="plan",
        )(wants, windows, r_tiles, own_tiles)

    def packed():
        return pl.pallas_call(
            functools.partial(pack_kernel, fine=fine, groups=groups, blocks=row_blocks),
            in_specs=[smem(), smem(), smem(), vmem(), anywhere()],
            out_specs=[anywhere(), anywhere(), vmem()],
            out_shape=[
                shape((PACK, size, size), BF16),
                shape((PACK, size, size), BF16),
                shape((1, LANES), I32),
            ],
            scratch_shapes=[
                pltpu.VMEM((8, LANES), I32),
                pltpu.SMEM((8, LANES), I32),
                pltpu.SemaphoreType.DMA,
                pltpu.SemaphoreType.DMA,
            ],
            compiler_params=limit(4),
            name="pack",
        )(above, below, wants, own_window, a_tiles)

    def product(low, high, side, whole, near):
        return pl.pallas_call(
            functools.partial(product_kernel, side=side, whole=whole),
            in_specs=[smem()] + [vmem()] * 4,
            out_specs=vmem(),
            out_shape=sums,
            compiler_params=limit(16),
            name="products",
        )(pairs, *near, low, high)

    def multiplied(low, high, whole, near):
        send = product(low, high, 0, whole, near)
        got = lax.ppermute(send, "core", [(0, 1), (1, 0)])
        keep = product(low, high, 1, whole, near)
        return keep, got

    def coded(keep, got):
        chunk = pl.BlockSpec((rows, size, size), lambda i: (i, 0, 0))
        return pl.pallas_call(
            code_kernel,
            grid=(chips,),
            in_specs=[chunk, chunk],
            out_specs=[
                pl.BlockSpec((rows, size, size), lambda i: (0, 0, 0)),
                pl.BlockSpec((1, coded_rows, size), lambda i: (i, 0, 0)),
            ],
            out_shape=[shape((rows, size, size), F32), shape((chips, coded_rows, size), jnp.int16)],
            compiler_params=limit(20),
            name="code",
        )(keep, got)

    def finish(own, codes):
        return pl.pallas_call(
            decode_kernel,
            in_specs=[vmem(), vmem()],
            out_specs=vmem(),
            out_shape=shape((rows, 1, size, size), BF16),
            compiler_params=limit(16),
            name="decode",
        )(own, codes)

    up, down, words = packed()
    low = lax.ppermute(up, ROWS, to_next)
    high = lax.ppermute(down, ROWS, to_last)
    shared = lax.all_to_all(jnp.broadcast_to(words[None], (firsts, 1, LANES)), FIRST, 0, 0, tiled=True)
    pairs, r_near, own_near = plan()
    own, codes = coded(*multiplied(low, high, False, (r_near, own_near)))
    codes = lax.all_to_all(codes, "x", 0, 0, tiled=True)
    shared = lax.psum(jnp.sum(shared, axis=0), SECOND)
    c_tiles = finish(own, codes)
    row_offsets, over = pl.pallas_call(
        functools.partial(offset_kernel, blocks=row_blocks),
        in_specs=[smem(), vmem()],
        out_specs=[smem(), smem()],
        out_shape=[shape((rows,), I32), shape((1,), I32)],
        compiler_params=limit(4),
        name="offsets",
    )(c_counts, shared)

    def redo(state):
        low = lax.ppermute(own_tiles, ROWS, to_next)
        high = lax.ppermute(own_tiles, ROWS, to_last)
        own, codes = coded(*multiplied(low, high, True, (r_tiles, own_tiles)))
        return jnp.int32(0), finish(own, lax.all_to_all(codes, "x", 0, 0, tiled=True))

    c_tiles = lax.while_loop(lambda state: state[0] > 0, redo, (over[0], c_tiles))[1]
    return (c_tiles, row_offsets)


def solution(mesh):
    finer = Mesh(mesh.devices.reshape(8, mesh.shape["rows"] // 8, mesh.shape["inner"] // 2, 2), EVERY)
    return jax.shard_map(
        body,
        mesh=finer,
        in_specs=(
            P(ROWS, INNER, None, None),
            P(ROWS, INNER),
            P(EVERY, None, None, None),
            P(),
            P(ROWS, None),
            P(ROWS),
        ),
        out_specs=(P(ROWS, INNER, None, None), P(ROWS)),
        check_vma=False,
    )
```

```python
import functools

import jax
import jax.numpy as jnp
from jax import lax
from jax.experimental import pallas as pl
from jax.experimental.pallas import tpu as pltpu
from jax.sharding import Mesh
from jax.sharding import PartitionSpec as P


I32 = jnp.int32
F32 = jnp.float32
BF16 = jnp.bfloat16
ROWS = ("r0", "r1")
INNER = ("x", "core")
EVERY = ROWS + INNER
FIRST = ("r1", "x", "core")
SECOND = "r0"
LANES = 128
PACK = 20
STEPS = 256.0
TOP = 32766.0
UNROLL = 4
HEAD = 8
HALF = 512


def slot_words(wants_ref, kinds, keys, count):
    for c in range(count):
        used = jnp.zeros_like(keys)
        fed = jnp.zeros_like(keys)
        for n in range(count):
            used = jnp.where(keys == wants_ref[c, n], n + 1, used)
            fed = jnp.where(kinds == wants_ref[count + c, n], n + 1, fed)
        yield c, used, fed


def plan_kernel(
    wants_ref, win_ref, r_ref, a_ref, list_ref, r_out, a_out, words, table, sem, load_sems, *, fine, groups, blocks
):
    loads = [
        pltpu.make_async_copy(r_ref, r_out, load_sems.at[0]),
        pltpu.make_async_copy(a_ref, a_out, load_sems.at[1]),
    ]
    for load in loads:
        load.start()
    slots = win_ref.shape[1]
    rows = wants_ref.shape[1]
    core = lax.axis_index("core")
    row = lax.axis_index(ROWS)
    group = lax.axis_index(INNER)
    lane = lax.broadcasted_iota(I32, (slots, LANES), 1)
    half = rows // 2
    for src in range(3):
        first = (row - 1 + src) * (groups * fine) + group * fine
        block = jnp.clip(lax.div(first + LANES, LANES) - 1, 0, blocks - 1)
        keys = block * LANES + lane
        own = (keys >= first) & (keys < first + fine)
        packed = [jnp.zeros((slots, LANES), I32), jnp.zeros((slots, LANES), I32)]
        for c, used, fed in slot_words(wants_ref, win_ref[src], keys, rows):
            code = jnp.where(own & (used > 0) & (fed > 0), (fed - 1) * rows + used, 0)
            packed[c // half] = packed[c // half] | (code << (7 * (c % half)))
        words[src, 0, :slots] = packed[0]
        words[src, 1, :slots] = packed[1]
        slot = lax.broadcasted_iota(I32, (slots, LANES), 0)
        marks = jnp.where((packed[0] | packed[1]) != 0, jnp.left_shift(1, slot), 0)
        words[src, 0, slots : slots + 1] = jnp.sum(marks, axis=0, keepdims=True)
    copy = pltpu.make_async_copy(words, table, sem)
    copy.start()
    copy.wait()

    n = (jnp.int32(HEAD), jnp.int32(HALF))
    for src in range(3):
        first = (row - 1 + src) * (groups * fine) + group * fine
        base = lax.rem(first + LANES, LANES)
        began = n

        def fine_row(q, carry, src=src, base=base):
            mark = table[src, 0, slots, base + q]

            def found(carry):
                for t in range(slots):

                    def pairs(carry, t=t):
                        sent, kept, place = carry
                        spot = (q * slots + t) * 64 + place
                        low = table[src, 0, t, base + q]
                        high = table[src, 1, t, base + q]
                        for c in range(rows):
                            code = (((low if c < half else high) >> (7 * (c % half))) & 127) - 1
                            mine = ((code >> 3) & 1) == core
                            list_ref[jnp.where(mine, kept, sent)] = spot * 512 + c * 64 + jnp.maximum(code, 0)
                            live = code >= 0
                            kept = kept + (live & mine).astype(I32)
                            sent = sent + (live & jnp.logical_not(mine)).astype(I32)
                        return sent, kept, place + 1

                    carry = lax.cond((mark & (1 << t)) != 0, pairs, lambda carry: carry, carry)
                return carry

            return lax.cond(mark != 0, found, lambda carry: carry, carry)

        n = lax.fori_loop(0, fine, fine_row, (*n, jnp.int32(0)))[:2]
        list_ref[src] = n[0] - began[0]
        list_ref[3 + src] = n[1] - began[1]
    for load in loads:
        load.wait()


def pack_kernel(
    up_ref, down_ref, wants_ref, win_ref, a_ref, up_out, down_out, told_ref, need, flags, sem, copy_sem, *, fine, groups, blocks
):
    slots = win_ref.shape[0]
    rows = up_ref.shape[1]
    pack = up_out.shape[0]
    row = lax.axis_index(ROWS)
    group = lax.axis_index(INNER)
    first = row * (groups * fine) + group * fine
    base = lax.rem(first, LANES)
    lane = lax.broadcasted_iota(I32, (slots, LANES), 1)
    slot = lax.broadcasted_iota(I32, (slots, LANES), 0)
    keys = first - base + lane
    own = (keys >= first) & (keys < first + fine)
    for side, ref in enumerate((up_ref, down_ref)):
        wanted = jnp.zeros((slots, LANES), I32)
        for _, used, fed in slot_words(ref, win_ref[...], keys, rows):
            wanted = jnp.where(own & (used > 0) & (fed > 0), jnp.left_shift(1, slot), wanted)
        need[side : side + 1] = jnp.sum(wanted, axis=0, keepdims=True)
    copy = pltpu.make_async_copy(need, flags, sem)
    copy.start()
    copy.wait()
    outs = (up_out, down_out)

    def fine_row(q, places):
        after = []
        for side in range(2):
            mark = flags[side, base + q]
            place = places[side]

            def found(place, side=side, mark=mark):
                for t in range(slots):
                    flag = lax.shift_right_logical(mark, t) & 1

                    @pl.when((flag > 0) & (place < pack))
                    def _(t=t, place=place):
                        pltpu.make_async_copy(a_ref.at[q, t], outs[side].at[place], copy_sem).start()

                    place = place + flag
                return place

            after.append(lax.cond(mark != 0, found, lambda place: place, place))
        return tuple(after)

    up_count, down_count = lax.fori_loop(0, fine, fine_row, (jnp.int32(0), jnp.int32(0)))

    total = wants_ref[2 * rows, 0]
    for c in range(1, rows):
        total = total + wants_ref[2 * rows, c]
    lane = lax.broadcasted_iota(I32, (1, LANES), 1)
    mine = jnp.where((lane == row) & (group == 0), total, 0)
    over = (jnp.maximum(up_count, down_count) > pack).astype(I32)
    words = jnp.where(lane == blocks, over, mine)
    told_ref[...] = words

    @pl.loop(0, jnp.minimum(up_count, pack) + jnp.minimum(down_count, pack))
    def _(i):
        pltpu.make_async_copy(a_ref.at[0, 0], up_out.at[0], copy_sem).wait()


def product_kernel(list_ref, r_ref, own_ref, low_ref, high_ref, out_ref, *, side, whole):
    pack = low_ref.shape[0]
    cells = out_ref.shape[0] - 1
    rows = r_ref.shape[0]

    @pl.loop(0, cells)
    def _(i):
        out_ref[i] = jnp.zeros(out_ref.shape[1:], F32)

    begin = jnp.int32(HALF if side else HEAD)
    for src, ref in enumerate((low_ref, own_ref, high_ref)):
        end = begin + list_ref[3 * side + src]

        @pl.loop(0, lax.div(end - begin + UNROLL - 1, UNROLL))
        def _(i, src=src, ref=ref, begin=begin, end=end):
            for u in range(UNROLL):
                at = begin + i * UNROLL + u
                entry = list_ref[at]
                spot = lax.shift_right_logical(entry, 15) & 63
                place = lax.shift_right_logical(entry, 9) & 63
                row = lax.shift_right_logical(entry, 6) & 7
                slot = lax.shift_right_logical(entry, 3) & 7
                live = at < end
                if src == 1 or whole:
                    place = spot
                else:
                    live = live & (place < pack)
                place = jnp.where(live, place, 0)
                cell = jnp.where(live, lax.shift_right_logical(slot, 1) * rows + row, cells)
                part = jnp.dot(r_ref[row, entry & 7], ref[place], preferred_element_type=F32)
                out_ref[cell] = out_ref[cell] + part

        begin = end


def code_kernel(keep_ref, got_ref, own_out, out, codes, sems):
    rows, size = own_out.shape[:2]
    chips = out.shape[0]
    chip = lax.axis_index("x")
    copies = []
    for d in range(1, chips):
        there = lax.rem(chip + d, chips)
        levels = []
        for c in range(rows):
            value = keep_ref[there * rows + c] + got_ref[there * rows + c]
            top = jnp.max(jnp.abs(value), axis=0, keepdims=True)
            level = jnp.ceil(jnp.log2(jnp.maximum(top, 1e-30)) * STEPS) + 1.0
            code = jnp.round(value * (jnp.exp2(level * (-1.0 / STEPS)) * TOP))
            codes[d - 1, pl.ds(c * size, size)] = code.astype(I32).astype(jnp.int16)
            levels.append(level)
        levels = jnp.concatenate(levels + levels, axis=0)
        codes[d - 1, pl.ds(rows * size, 2 * rows)] = levels.astype(I32).astype(jnp.int16)
        copies.append(pltpu.make_async_copy(codes.at[d - 1], out.at[there], sems.at[d - 1]))
        copies[-1].start()
    for c in range(rows):
        own_out[c] = keep_ref[chip * rows + c] + got_ref[chip * rows + c]
    for copy in copies:
        copy.wait()


def decode_kernel(own_ref, code_ref, out_ref):
    rows = out_ref.shape[0]
    size = out_ref.shape[2]
    chips = code_ref.shape[0]
    chip = lax.axis_index("x")
    parts = [lax.rem(chip + d, chips) for d in range(1, chips)]
    scales = [
        jnp.exp2(code_ref[p, pl.ds(rows * size, 2 * rows)].astype(F32) * (1.0 / STEPS)) * (1.0 / TOP) for p in parts
    ]
    for c in range(rows):
        total = own_ref[c]
        for p, scale in zip(parts, scales):
            total = total + code_ref[p, pl.ds(c * size, size)].astype(F32) * scale[c : c + 1]
        out_ref[c, 0] = total.astype(BF16)


def offset_kernel(counts_ref, parts_ref, out_ref, over_ref, *, blocks):
    row = lax.axis_index(ROWS)
    words = parts_ref[...]
    lane = lax.broadcasted_iota(I32, words.shape, 1)
    over_ref[0] = jnp.sum(jnp.where(lane == blocks, words, 0))
    offset = jnp.sum(jnp.where(lane < row, words, 0))
    for c in range(out_ref.shape[0]):
        out_ref[c] = offset
        offset = offset + counts_ref[c]


def smem():
    return pl.BlockSpec(memory_space=pltpu.SMEM)


def vmem():
    return pl.BlockSpec(memory_space=pltpu.VMEM)


def anywhere():
    return pl.BlockSpec(memory_space=pl.ANY)


def shape(dims, dtype):
    return jax.ShapeDtypeStruct(dims, dtype)


def body(r_tiles, r_cols, a_tiles, a_cols, c_cols, c_counts):
    fine, op_slots, size, _ = a_tiles.shape
    rows, _ = r_tiles.shape[:2]
    groups = lax.axis_size(INNER)
    chips = lax.axis_size("x")
    row_blocks = lax.axis_size(ROWS)
    row = lax.axis_index(ROWS)
    group = lax.axis_index(INNER)
    blocks = a_cols.shape[0] // LANES
    limit = lambda mb: pltpu.CompilerParams(vmem_limit_bytes=mb * 2**20)

    to_next = [(i, i + 1) for i in range(row_blocks - 1)]
    to_last = [(i + 1, i) for i in range(row_blocks - 1)]

    wants = jnp.concatenate([r_cols, c_cols, c_counts[None]])
    below = lax.ppermute(wants, ROWS, to_next)
    above = lax.ppermute(wants, ROWS, to_last)

    by_slot = a_cols.T

    def window(block_row):
        first = block_row * (groups * fine) + group * fine
        block = jnp.clip((first + LANES) // LANES - 1, 0, blocks - 1)
        return lax.dynamic_slice(by_slot, (0, block * LANES), (op_slots, LANES))

    own_window = window(row)
    windows = jnp.stack([window(row - 1), own_window, window(row + 1)])
    firsts = lax.axis_size(FIRST)
    own_tiles = a_tiles.reshape(fine * op_slots, size, size)
    sums = shape((chips * rows + 1, size, size), F32)
    coded_rows = rows * size + 2 * rows

    def plan():
        return pl.pallas_call(
            functools.partial(plan_kernel, fine=fine, groups=groups, blocks=blocks),
            in_specs=[smem(), vmem(), anywhere(), anywhere()],
            out_specs=[smem(), vmem(), vmem()],
            out_shape=[
                shape((2 * HALF,), I32),
                pltpu.VMEM(r_tiles.shape, BF16),
                pltpu.VMEM(own_tiles.shape, BF16),
            ],
            scratch_shapes=[
                pltpu.VMEM((3, 2, 8, LANES), I32),
                pltpu.SMEM((3, 2, 8, LANES), I32),
                pltpu.SemaphoreType.DMA,
                pltpu.SemaphoreType.DMA((2,)),
            ],
            compiler_params=limit(8),
            name="plan",
        )(wants, windows, r_tiles, own_tiles)

    def packed():
        return pl.pallas_call(
            functools.partial(pack_kernel, fine=fine, groups=groups, blocks=row_blocks),
            in_specs=[smem(), smem(), smem(), vmem(), anywhere()],
            out_specs=[anywhere(), anywhere(), vmem()],
            out_shape=[
                shape((PACK, size, size), BF16),
                shape((PACK, size, size), BF16),
                shape((1, LANES), I32),
            ],
            scratch_shapes=[
                pltpu.VMEM((8, LANES), I32),
                pltpu.SMEM((8, LANES), I32),
                pltpu.SemaphoreType.DMA,
                pltpu.SemaphoreType.DMA,
            ],
            compiler_params=limit(4),
            name="pack",
        )(above, below, wants, own_window, a_tiles)

    def product(low, high, side, whole, near):
        return pl.pallas_call(
            functools.partial(product_kernel, side=side, whole=whole),
            in_specs=[smem()] + [vmem()] * 4,
            out_specs=vmem(),
            out_shape=sums,
            compiler_params=limit(16),
            name="products",
        )(pairs, *near, low, high)

    def multiplied(low, high, whole, near):
        send = product(low, high, 0, whole, near)
        got = lax.ppermute(send, "core", [(0, 1), (1, 0)])
        keep = product(low, high, 1, whole, near)
        return keep, got

    def coded(keep, got):
        return pl.pallas_call(
            code_kernel,
            in_specs=[vmem(), vmem()],
            out_specs=[vmem(), anywhere()],
            out_shape=[shape((rows, size, size), F32), shape((chips, coded_rows, size), jnp.int16)],
            scratch_shapes=[
                pltpu.VMEM((chips - 1, coded_rows, size), jnp.int16),
                pltpu.SemaphoreType.DMA((chips - 1,)),
            ],
            compiler_params=limit(16),
            name="code",
        )(keep, got)

    def finish(own, codes):
        return pl.pallas_call(
            decode_kernel,
            in_specs=[vmem(), vmem()],
            out_specs=vmem(),
            out_shape=shape((rows, 1, size, size), BF16),
            compiler_params=limit(16),
            name="decode",
        )(own, codes)

    up, down, words = packed()
    low = lax.ppermute(up, ROWS, to_next)
    high = lax.ppermute(down, ROWS, to_last)
    shared = lax.all_to_all(jnp.broadcast_to(words[None], (firsts, 1, LANES)), FIRST, 0, 0, tiled=True)
    pairs, r_near, own_near = plan()
    own, codes = coded(*multiplied(low, high, False, (r_near, own_near)))
    codes = lax.all_to_all(codes, "x", 0, 0, tiled=True)
    shared = lax.psum(jnp.sum(shared, axis=0), SECOND)
    c_tiles = finish(own, codes)
    row_offsets, over = pl.pallas_call(
        functools.partial(offset_kernel, blocks=row_blocks),
        in_specs=[smem(), vmem()],
        out_specs=[smem(), smem()],
        out_shape=[shape((rows,), I32), shape((1,), I32)],
        compiler_params=limit(4),
        name="offsets",
    )(c_counts, shared)

    def redo(state):
        low = lax.ppermute(own_tiles, ROWS, to_next)
        high = lax.ppermute(own_tiles, ROWS, to_last)
        own, codes = coded(*multiplied(low, high, True, (r_tiles, own_tiles)))
        return jnp.int32(0), finish(own, lax.all_to_all(codes, "x", 0, 0, tiled=True))

    c_tiles = lax.while_loop(lambda state: state[0] > 0, redo, (over[0], c_tiles))[1]
    return (c_tiles, row_offsets)


def solution(mesh):
    finer = Mesh(mesh.devices.reshape(8, mesh.shape["rows"] // 8, mesh.shape["inner"] // 2, 2), EVERY)
    return jax.shard_map(
        body,
        mesh=finer,
        in_specs=(
            P(ROWS, INNER, None, None),
            P(ROWS, INNER),
            P(EVERY, None, None, None),
            P(),
            P(ROWS, None),
            P(ROWS),
        ),
        out_specs=(P(ROWS, INNER, None, None), P(ROWS)),
        check_vma=False,
    )
```
